16 devices in a mesh: ep: 16 (over z, y, x, core).
Axes of the slice: x: 2, y: 2, z: 2, core: 2. Of those that a mesh axis runs over, the one named last changes fastest.
Arguments:
- tokens: bfloat16 [2048, 4096], P('ep')
- k_cache: bfloat16 [2048, 128, 8, 128], P('ep')
- v_cache: bfloat16 [2048, 128, 8, 128], P('ep')
- positions: int32 [2048], P('ep')
- expert_one: int32 [2048], P('ep')
- expert_two: int32 [2048], P('ep')
- eligible: int32 [2048, 16], P('ep')
- ln1_gain: bfloat16 [4096], replicated
- ln1_bias: bfloat16 [4096], replicated
- w_query: bfloat16 [4096, 4096], replicated
- b_query: bfloat16 [4096], replicated
- w_key: bfloat16 [4096, 1024], replicated
- b_key: bfloat16 [1024], replicated
- w_value: bfloat16 [4096, 1024], replicated
- b_value: bfloat16 [1024], replicated
- w_out: bfloat16 [4096, 4096], replicated
- b_out: bfloat16 [4096], replicated
- ln2_gain: bfloat16 [4096], replicated
- ln2_bias: bfloat16 [4096], replicated
- w_router: bfloat16 [4096, 16], replicated
- w_gate: bfloat16 [16, 4096, 960], P('ep')
- w_up: bfloat16 [16, 4096, 960], P('ep')
- w_down: bfloat16 [16, 960, 4096], P('ep')
Outputs:
- output 1: bfloat16 [2048, 4096], P('ep')
- output 2: bfloat16 [2048, 8, 128], P('ep')
- output 3: bfloat16 [2048, 8, 128], P('ep')
All inputs are finite; a program needn't handle non-finite values.
Results may differ from the reference program's by a relative error of at most 0.00965712.
Values are sent between devices in bfloat16 or wider.
A program may use at most 1 GiB of HBM per device.

```python
import jax
import jax.numpy as jnp
from jax import lax

D_MODEL = 4096
NUM_HEADS = 32
NUM_KV_HEADS = 8
HEAD_DIM = 128
FF_DIM = 960
NUM_EXPERTS = 16
TOK_DEV = 128
SEQ_LEN = 128
NUM_GROUPS = 16
BATCH = TOK_DEV * NUM_GROUPS
GROUP_SIZE = NUM_HEADS // NUM_KV_HEADS
Q_DIM = NUM_HEADS * HEAD_DIM
KV_DIM = NUM_KV_HEADS * HEAD_DIM
ROPE_BASE = 10000.0
LN_EPS = 1e-5


def draw_normal(key, arr_shape, std_dev):
    return (jax.random.normal(key, arr_shape, jnp.float32) * std_dev).astype(jnp.bfloat16)


def draw_positions(key):
    k_pos, k_top, k_low = jax.random.split(key, 3)
    row_ids = jnp.arange(BATCH)
    pos_vals = jax.random.randint(k_pos, (BATCH,), 0, SEQ_LEN)
    top_row = jax.random.randint(k_top, (), 0, BATCH)
    low_row = (top_row + 1 + jax.random.randint(k_low, (), 0, BATCH - 1)) % BATCH
    pos_vals = jnp.where(row_ids == top_row, SEQ_LEN - 1, pos_vals)
    return jnp.where(row_ids == low_row, 0, pos_vals).astype(jnp.int32)


def draw_routes(key):
    k_mix, k_hot, k_src, k_rot, k_sec, k_elig = jax.random.split(key, 6)
    row_ids = jnp.arange(BATCH)
    mix_draw = jax.random.randint(k_mix, (BATCH,), 0, 4 * NUM_EXPERTS)
    hot_expert = jax.random.randint(k_hot, (), 0, NUM_EXPERTS)
    first_choice = jnp.where(mix_draw < 2 * NUM_EXPERTS, mix_draw % NUM_EXPERTS, (hot_expert + mix_draw % 2) % NUM_EXPERTS)
    src_group = jax.random.randint(k_src, (), 0, NUM_GROUPS)
    first_choice = jnp.where(row_ids // TOK_DEV == src_group, hot_expert, first_choice)
    rotation = jax.random.randint(k_rot, (), 0, NUM_EXPERTS)
    offset_rows = (row_ids - (src_group + 1) * TOK_DEV) % BATCH
    first_choice = jnp.where(offset_rows < NUM_EXPERTS, (offset_rows + rotation) % NUM_EXPERTS, first_choice)
    second_choice = (first_choice + 1 + jax.random.randint(k_sec, (BATCH,), 0, NUM_EXPERTS - 1)) % NUM_EXPERTS
    expert_ids = jnp.arange(NUM_EXPERTS)[None, :]
    extra_elig = jax.random.randint(k_elig, (BATCH, NUM_EXPERTS), 0, 8) == 0
    eligible = extra_elig | (expert_ids == first_choice[:, None]) | (expert_ids == second_choice[:, None])
    return first_choice.astype(jnp.int32), second_choice.astype(jnp.int32), eligible.astype(jnp.int32)


def setup_inputs(seed: int = 0) -> dict:
    keys = jax.random.split(jax.random.key(seed), 22)
    expert_one, expert_two, eligible = draw_routes(keys[0])
    value_mean = jax.random.normal(keys[3], (BATCH, 1, NUM_KV_HEADS, HEAD_DIM), jnp.float32)
    value_draw = jax.random.normal(keys[4], (BATCH, SEQ_LEN, NUM_KV_HEADS, HEAD_DIM), jnp.float32)
    ln1_gain = (1.0 + 0.3 * jax.random.normal(keys[6], (D_MODEL,), jnp.float32)).astype(jnp.bfloat16)
    ln2_gain = (1.0 + 0.3 * jax.random.normal(keys[16], (D_MODEL,), jnp.float32)).astype(jnp.bfloat16)
    return {
        'tokens': draw_normal(keys[1], (BATCH, D_MODEL), 1.0),
        'k_cache': draw_normal(keys[2], (BATCH, SEQ_LEN, NUM_KV_HEADS, HEAD_DIM), 2.0),
        'v_cache': (value_draw + value_mean).astype(jnp.bfloat16),
        'positions': draw_positions(keys[5]),
        'expert_one': expert_one,
        'expert_two': expert_two,
        'eligible': eligible,
        'ln1_gain': ln1_gain,
        'ln1_bias': draw_normal(keys[7], (D_MODEL,), 0.3),
        'w_query': draw_normal(keys[8], (D_MODEL, Q_DIM), D_MODEL ** -0.5),
        'b_query': draw_normal(keys[9], (Q_DIM,), 0.5),
        'w_key': draw_normal(keys[10], (D_MODEL, KV_DIM), D_MODEL ** -0.5),
        'b_key': draw_normal(keys[11], (KV_DIM,), 0.5),
        'w_value': draw_normal(keys[12], (D_MODEL, KV_DIM), D_MODEL ** -0.5),
        'b_value': draw_normal(keys[13], (KV_DIM,), 0.5),
        'w_out': draw_normal(keys[14], (Q_DIM, D_MODEL), Q_DIM ** -0.5),
        'b_out': draw_normal(keys[15], (D_MODEL,), 0.3),
        'ln2_gain': ln2_gain,
        'ln2_bias': draw_normal(keys[17], (D_MODEL,), 0.3),
        'w_router': draw_normal(keys[18], (D_MODEL, NUM_EXPERTS), D_MODEL ** -0.5),
        'w_gate': draw_normal(keys[19], (NUM_EXPERTS, D_MODEL, FF_DIM), D_MODEL ** -0.5),
        'w_up': draw_normal(keys[20], (NUM_EXPERTS, D_MODEL, FF_DIM), D_MODEL ** -0.5),
        'w_down': draw_normal(keys[21], (NUM_EXPERTS, FF_DIM, D_MODEL), FF_DIM ** -0.5),
    }


def layer_norm(values_in, gain, bias):
    mean_val = jnp.mean(values_in, axis=-1, keepdims=True)
    centered = values_in - mean_val
    var_val = jnp.mean(centered * centered, axis=-1, keepdims=True)
    return centered * lax.rsqrt(var_val + LN_EPS) * gain.astype(jnp.float32) + bias.astype(jnp.float32)


def rope_tables(positions):
    half_dim = HEAD_DIM // 2
    inv_freq = ROPE_BASE ** (jnp.arange(half_dim, dtype=jnp.float32) * (-2.0 / HEAD_DIM))
    angles = positions.astype(jnp.float32)[:, None] * inv_freq[None, :]
    angles = jnp.concatenate([angles, angles], axis=-1)
    return jnp.cos(angles), jnp.sin(angles)


def apply_rope(values_in, cos_tab, sin_tab):
    half_dim = values_in.shape[-1] // 2
    rotated = jnp.concatenate([-values_in[..., half_dim:], values_in[..., :half_dim]], axis=-1)
    return values_in * cos_tab[:, None, :] + rotated * sin_tab[:, None, :]


def attend_one(seq_parts):
    q_seq, k_seq, v_seq, k_one, v_one, pos_one = seq_parts
    score_scale = HEAD_DIM ** -0.5
    q_f = q_seq.astype(jnp.float32)
    s_cache = jnp.einsum('kgd,skd->kgs', q_f, k_seq.astype(jnp.float32)) * score_scale
    valid_mask = jnp.arange(SEQ_LEN)[None, None, :] < pos_one
    s_cache = jnp.where(valid_mask, s_cache, -jnp.inf)
    s_new = jnp.einsum('kgd,kd->kg', q_f, k_one.astype(jnp.float32)) * score_scale
    top_val = jnp.maximum(jnp.max(s_cache, axis=-1), s_new)
    e_cache = jnp.exp(s_cache - top_val[..., None])
    e_new = jnp.exp(s_new - top_val)
    denom_sum = jnp.sum(e_cache, axis=-1) + e_new
    p_cache = (e_cache / denom_sum[..., None]).astype(jnp.bfloat16).astype(jnp.float32)
    p_new = (e_new / denom_sum).astype(jnp.bfloat16).astype(jnp.float32)
    attn_vals = jnp.einsum('kgs,skd->kgd', p_cache, v_seq.astype(jnp.float32))
    return attn_vals + p_new[..., None] * v_one.astype(jnp.float32)[:, None, :]


def router_gates(h_two, w_router, expert_one, expert_two, eligible):
    logits = jnp.dot(h_two, w_router, preferred_element_type=jnp.float32)
    expert_ids = jnp.arange(NUM_EXPERTS)[None, :]
    hit_one = expert_ids == expert_one[:, None]
    hit_two = expert_ids == expert_two[:, None]
    keep_one = eligible == 1
    keep_two = keep_one & jnp.logical_not(hit_one)
    prob_one = jax.nn.softmax(jnp.where(keep_one, logits, -jnp.inf), axis=-1)
    prob_two = jax.nn.softmax(jnp.where(keep_two, logits, -jnp.inf), axis=-1)
    gate_one = jnp.sum(jnp.where(hit_one, prob_one, 0.0), axis=-1)
    gate_two = jnp.sum(jnp.where(hit_two, prob_two, 0.0), axis=-1)
    return gate_one, gate_two


def reference(tokens, k_cache, v_cache, positions, expert_one, expert_two, eligible, ln1_gain, ln1_bias, w_query, b_query, w_key, b_key, w_value, b_value, w_out, b_out, ln2_gain, ln2_bias, w_router, w_gate, w_up, w_down):
    x_f = tokens.astype(jnp.float32)
    h_one = layer_norm(x_f, ln1_gain, ln1_bias).astype(jnp.bfloat16)
    cos_tab, sin_tab = rope_tables(positions)
    q_lin = jnp.dot(h_one, w_query, preferred_element_type=jnp.float32) + b_query.astype(jnp.float32)
    q_rot = apply_rope(q_lin.reshape(BATCH, NUM_HEADS, HEAD_DIM), cos_tab, sin_tab).astype(jnp.bfloat16)
    k_lin = jnp.dot(h_one, w_key, preferred_element_type=jnp.float32) + b_key.astype(jnp.float32)
    key_new = apply_rope(k_lin.reshape(BATCH, NUM_KV_HEADS, HEAD_DIM), cos_tab, sin_tab).astype(jnp.bfloat16)
    v_lin = jnp.dot(h_one, w_value, preferred_element_type=jnp.float32) + b_value.astype(jnp.float32)
    value_new = v_lin.astype(jnp.bfloat16).reshape(BATCH, NUM_KV_HEADS, HEAD_DIM)
    q_grp = q_rot.reshape(BATCH, NUM_KV_HEADS, GROUP_SIZE, HEAD_DIM)
    attn_vals = lax.map(attend_one, (q_grp, k_cache, v_cache, key_new, value_new, positions))
    attn_flat = attn_vals.astype(jnp.bfloat16).reshape(BATCH, Q_DIM)
    x_mid = (x_f + jnp.dot(attn_flat, w_out, preferred_element_type=jnp.float32) + b_out.astype(jnp.float32)).astype(jnp.bfloat16)
    h_two = layer_norm(x_mid.astype(jnp.float32), ln2_gain, ln2_bias).astype(jnp.bfloat16)
    gate_one, gate_two = router_gates(h_two, w_router, expert_one, expert_two, eligible)

    def expert_step(acc_sum, expert_parts):
        gate_w, up_w, down_w, expert_idx = expert_parts
        u_val = jnp.dot(h_two, gate_w, preferred_element_type=jnp.float32)
        v_val = jnp.dot(h_two, up_w, preferred_element_type=jnp.float32)
        z_val = (jax.nn.silu(u_val) * v_val).astype(jnp.bfloat16)
        out_val = jnp.dot(z_val, down_w, preferred_element_type=jnp.float32).astype(jnp.bfloat16)
        weight_col = jnp.where(expert_one == expert_idx, gate_one, 0.0) + jnp.where(expert_two == expert_idx, gate_two, 0.0)
        return acc_sum + weight_col[:, None] * out_val.astype(jnp.float32), None

    y_sum, _ = lax.scan(expert_step, jnp.zeros((BATCH, D_MODEL), jnp.float32), (w_gate, w_up, w_down, jnp.arange(NUM_EXPERTS)))
    tokens_out = (x_mid.astype(jnp.float32) + y_sum).astype(jnp.bfloat16)
    return tokens_out, key_new, value_new
```

```python
import functools

import jax
import jax.numpy as jnp
from jax import lax
from jax.experimental import pallas as pl
from jax.experimental.pallas import tpu as pltpu
from jax.sharding import PartitionSpec as P

ROPE_BASE = 10000.0
LN_EPS = 1e-5
CHUNKS = 2
MIB = 1024 * 1024


def layer_norm_rows(x, gain, bias):
    mean_val = jnp.mean(x, axis=-1, keepdims=True)
    centered = x - mean_val
    var_val = jnp.mean(centered * centered, axis=-1, keepdims=True)
    return centered * lax.rsqrt(var_val + LN_EPS) * gain + bias


def rope_tables(positions, head_dim):
    half_dim = head_dim // 2
    inv_freq = ROPE_BASE ** (jnp.arange(half_dim, dtype=jnp.float32) * (-2.0 / head_dim))
    angles = positions.astype(jnp.float32)[:, None] * inv_freq[None, :]
    cos_val, sin_val = jnp.cos(angles), jnp.sin(angles)
    return jnp.concatenate([cos_val, cos_val], axis=-1), jnp.concatenate([-sin_val, sin_val], axis=-1)


def qkv_kernel(head_dim, q_steps, kv_steps, tok_ref, gain_ref, bias_ref, cos_ref, sin_ref, wq_ref, wk_ref, wv_ref, bq_ref, bk_ref, bv_ref, q_ref, k_ref, v_ref, h_ref):
    step = pl.program_id(0)

    @pl.when(step == 0)
    def _():
        x = tok_ref[...].astype(jnp.float32)
        h_ref[...] = layer_norm_rows(x, gain_ref[...].astype(jnp.float32), bias_ref[...].astype(jnp.float32)).astype(jnp.bfloat16)

    def project(w_ref, b_ref):
        return jnp.dot(h_ref[...], w_ref[...], preferred_element_type=jnp.float32) + b_ref[...].astype(jnp.float32)

    def rotated(y, out_ref):
        for head in range(y.shape[1] // head_dim):
            cols = slice(head * head_dim, (head + 1) * head_dim)
            part = y[:, cols]
            turned = pltpu.roll(part, head_dim // 2, 1)
            out_ref[:, cols] = (part * cos_ref[...] + turned * sin_ref[...]).astype(jnp.bfloat16)

    @pl.when(step < q_steps)
    def _():
        rotated(project(wq_ref, bq_ref), q_ref)

    @pl.when((step >= q_steps) & (step < q_steps + kv_steps))
    def _():
        rotated(project(wk_ref, bk_ref), k_ref)

    @pl.when(step >= q_steps + kv_steps)
    def _():
        v_ref[...] = project(wv_ref, bv_ref).astype(jnp.bfloat16)


def qkv_project(tokens, gain, bias, cos_tab, sin_tab, w_query, w_key, w_value, b_query, b_key, b_value, head_dim):
    rows, d_model = tokens.shape
    q_dim, kv_dim = w_query.shape[1], w_key.shape[1]
    block = 512
    q_steps, kv_steps = q_dim // block, kv_dim // block

    def q_idx(i):
        return (0, jnp.minimum(i, q_steps - 1))

    def k_idx(i):
        return (0, jnp.clip(i - q_steps, 0, kv_steps - 1))

    def v_idx(i):
        return (0, jnp.clip(i - q_steps - kv_steps, 0, kv_steps - 1))

    def whole(arr):
        return pl.BlockSpec(arr.shape, lambda i: (0,) * arr.ndim)

    gain, bias = gain[None, :], bias[None, :]
    return pl.pallas_call(
        functools.partial(qkv_kernel, head_dim, q_steps, kv_steps),
        grid=(q_steps + 2 * kv_steps,),
        in_specs=[
            whole(tokens), whole(gain), whole(bias), whole(cos_tab), whole(sin_tab),
            pl.BlockSpec((d_model, block), q_idx), pl.BlockSpec((d_model, block), k_idx), pl.BlockSpec((d_model, block), v_idx),
            pl.BlockSpec((1, block), q_idx), pl.BlockSpec((1, block), k_idx), pl.BlockSpec((1, block), v_idx),
        ],
        out_specs=[pl.BlockSpec((rows, block), q_idx), pl.BlockSpec((rows, block), k_idx), pl.BlockSpec((rows, block), v_idx)],
        out_shape=[jax.ShapeDtypeStruct((rows, q_dim), jnp.bfloat16), jax.ShapeDtypeStruct((rows, kv_dim), jnp.bfloat16), jax.ShapeDtypeStruct((rows, kv_dim), jnp.bfloat16)],
        scratch_shapes=[pltpu.VMEM((rows, d_model), jnp.bfloat16)],
        compiler_params=pltpu.CompilerParams(dimension_semantics=("arbitrary",), vmem_limit_bytes=40 * MIB),
        cost_estimate=pl.CostEstimate(flops=2 * rows * d_model * (q_dim + 2 * kv_dim), bytes_accessed=2 * d_model * (q_dim + 2 * kv_dim), transcendentals=0),
    )(tokens, gain, bias, cos_tab, sin_tab, w_query, w_key, w_value, b_query[None, :], b_key[None, :], b_value[None, :])


def attend_kernel(batch, ahead, kv_heads, group_size, pos_ref, q_ref, kn_ref, vn_ref, k_hbm, v_hbm, out_ref, k_buf, v_buf, where_ref, k_sem, v_sem):
    tok_count, seq_len = k_hbm.shape[0], k_hbm.shape[1]
    num_heads, head_dim = q_ref.shape[1], q_ref.shape[2]
    rounds = tok_count // batch
    slots = ahead + 1
    cols = seq_len * kv_heads
    v_buf[...] = jnp.zeros_like(v_buf)
    col_ids = lax.broadcasted_iota(jnp.int32, (num_heads, cols), 1)
    head_ids = lax.broadcasted_iota(jnp.int32, (num_heads, cols), 0)
    where_ref[...] = jnp.where(col_ids % kv_heads == head_ids // group_size, col_ids // kv_heads, seq_len)

    def copies(turn, lane):
        tok = turn * batch + lane
        slot = lax.rem(turn, slots)
        count = ((pos_ref[tok] + 7) // 8) * 8
        k_copy = pltpu.make_async_copy(k_hbm.at[tok, pl.ds(0, count)], k_buf.at[slot, lane, pl.ds(0, count)], k_sem.at[slot])
        v_copy = pltpu.make_async_copy(v_hbm.at[tok, pl.ds(0, count)], v_buf.at[slot, lane, pl.ds(0, count)], v_sem.at[slot])
        return k_copy, v_copy

    def fetch(turn):
        for lane in range(batch):
            for copy in copies(turn, lane):
                copy.start()

    for turn in range(ahead):
        fetch(turn)

    scale = head_dim ** -0.5

    def one_round(turn, carry):
        @pl.when(turn + ahead < rounds)
        def _():
            fetch(turn + ahead)

        slot = lax.rem(turn, slots)
        for lane in range(batch):
            for copy in copies(turn, lane):
                copy.wait()
        for lane in range(batch):
            tok = turn * batch + lane
            pos = pos_ref[tok]
            k_buf[slot, lane, pos] = kn_ref[tok]
            v_buf[slot, lane, pos] = vn_ref[tok]
        for lane in range(batch):
            tok = turn * batch + lane
            pos = pos_ref[tok]
            k_all = k_buf[slot, lane].reshape(cols, head_dim)
            v_all = v_buf[slot, lane].reshape(cols, head_dim)
            s_val = lax.dot_general(q_ref[tok], k_all, (((1,), (1,)), ((), ())), preferred_element_type=jnp.float32) * scale
            s_val = jnp.where(where_ref[...] <= pos, s_val, -jnp.inf)
            e_val = jnp.exp(s_val - jnp.max(s_val, axis=-1, keepdims=True))
            p_val = (e_val * (1.0 / jnp.sum(e_val, axis=-1, keepdims=True))).astype(jnp.bfloat16)
            out_ref[tok] = jnp.dot(p_val, v_all, preferred_element_type=jnp.float32).astype(jnp.bfloat16)
        return carry

    lax.fori_loop(0, rounds, one_round, 0)


def attend(positions, q_heads, key_new, value_new, k_cache, v_cache):
    tok_count, seq_len, kv_heads, head_dim = k_cache.shape
    num_heads = q_heads.shape[1]
    batch, ahead = 4, 3
    buf = pltpu.VMEM((ahead + 1, batch, seq_len, kv_heads, head_dim), jnp.bfloat16)
    vmem = pl.BlockSpec(memory_space=pltpu.VMEM)
    return pl.pallas_call(
        functools.partial(attend_kernel, batch, ahead, kv_heads, num_heads // kv_heads),
        in_specs=[pl.BlockSpec(memory_space=pltpu.SMEM), vmem, vmem, vmem, pl.BlockSpec(memory_space=pltpu.HBM), pl.BlockSpec(memory_space=pltpu.HBM)],
        out_specs=vmem,
        out_shape=jax.ShapeDtypeStruct(q_heads.shape, jnp.bfloat16),
        scratch_shapes=[buf, buf, pltpu.VMEM((num_heads, seq_len * kv_heads), jnp.int32), pltpu.SemaphoreType.DMA((ahead + 1,)), pltpu.SemaphoreType.DMA((ahead + 1,))],
        compiler_params=pltpu.CompilerParams(vmem_limit_bytes=32 * MIB),
        cost_estimate=pl.CostEstimate(flops=4 * tok_count * num_heads * seq_len * kv_heads * head_dim, bytes_accessed=4 * k_cache.size, transcendentals=0),
    )(positions, q_heads, key_new, value_new, k_cache, v_cache)


def post_kernel(num_experts, steps, attn_ref, wo_ref, bo_ref, tok_ref, gain_ref, bias_ref, wr_ref, one_ref, two_ref, elig_ref, x_ref, send_ref, acc_ref):
    step = pl.program_id(0)
    block = wo_ref.shape[1]
    cols = pl.ds(pl.multiple_of(step * block, block), block)
    mixed = jnp.dot(attn_ref[...], wo_ref[...], preferred_element_type=jnp.float32)
    x_mid = (tok_ref[...].astype(jnp.float32) + mixed + bo_ref[...].astype(jnp.float32)).astype(jnp.bfloat16)
    x_ref[...] = x_mid
    acc_ref[:, cols] = x_mid

    @pl.when(step == steps - 1)
    def _():
        h_two = layer_norm_rows(acc_ref[...].astype(jnp.float32), gain_ref[...].astype(jnp.float32), bias_ref[...].astype(jnp.float32)).astype(jnp.bfloat16)
        logits = jnp.dot(h_two, wr_ref[...], preferred_element_type=jnp.float32)
        rows, width = logits.shape
        lanes = lax.broadcasted_iota(jnp.int32, (rows, width), 1)
        hit_one = lanes == one_ref[...]
        hit_two = lanes == two_ref[...]
        keep_one = elig_ref[...] == 1
        keep_two = keep_one & jnp.logical_not(hit_one)

        def gate(keep, hit):
            masked = jnp.where(keep, logits, -jnp.inf)
            e_val = jnp.exp(masked - jnp.max(masked, axis=-1, keepdims=True))
            return jnp.sum(jnp.where(hit, e_val, 0.0), axis=-1, keepdims=True) / jnp.sum(e_val, axis=-1, keepdims=True)

        gates = jnp.where(hit_one, gate(keep_one, hit_one), 0.0) + jnp.where(hit_two, gate(keep_two, hit_two), 0.0)
        high = gates.astype(jnp.bfloat16).astype(jnp.float32)
        rest = gates - high
        mid = rest.astype(jnp.bfloat16).astype(jnp.float32)
        packed = high + pltpu.roll(mid, num_experts, 1) + pltpu.roll(rest - mid, 2 * num_experts, 1)
        d_model = h_two.shape[1]
        send_ref[:, :d_model] = h_two
        send_ref[:, d_model:] = packed.astype(jnp.bfloat16)


def post_attention(attn, w_out, b_out, tokens, gain, bias, w_router, expert_one, expert_two, eligible):
    rows, d_model = tokens.shape
    num_experts = w_router.shape[1]
    width = 128
    block = 512
    steps = d_model // block
    w_router = jnp.pad(w_router, ((0, 0), (0, width - num_experts)))
    eligible = jnp.pad(eligible, ((0, 0), (0, width - num_experts)))
    one, two = expert_one[:, None], expert_two[:, None]
    gain, bias = gain[None, :], bias[None, :]

    def whole(arr):
        return pl.BlockSpec(arr.shape, lambda i: (0,) * arr.ndim)

    def col(i):
        return (0, i)

    return pl.pallas_call(
        functools.partial(post_kernel, num_experts, steps),
        grid=(steps,),
        in_specs=[
            whole(attn), pl.BlockSpec((attn.shape[1], block), col), pl.BlockSpec((1, block), col), pl.BlockSpec((rows, block), col),
            whole(gain), whole(bias), whole(w_router), whole(one), whole(two), whole(eligible),
        ],
        out_specs=[pl.BlockSpec((rows, block), col), pl.BlockSpec((rows, d_model + width), lambda i: (0, 0))],
        out_shape=[jax.ShapeDtypeStruct((rows, d_model), jnp.bfloat16), jax.ShapeDtypeStruct((rows, d_model + width), jnp.bfloat16)],
        scratch_shapes=[pltpu.VMEM((rows, d_model), jnp.bfloat16)],
        compiler_params=pltpu.CompilerParams(dimension_semantics=("arbitrary",), vmem_limit_bytes=48 * MIB),
        cost_estimate=pl.CostEstimate(flops=2 * rows * d_model * d_model, bytes_accessed=2 * d_model * d_model, transcendentals=0),
    )(attn, w_out, b_out[None, :], tokens, gain, bias, w_router, one, two, eligible)


def expert_kernel(num_experts, x_ref, wg_ref, wu_ref, wd_ref, y_ref):
    d_model = y_ref.shape[1]
    me = lax.axis_index('ep')
    x_val = x_ref[:, :d_model]
    packed = x_ref[:, d_model:].astype(jnp.float32)
    lanes = lax.broadcasted_iota(jnp.int32, packed.shape, 1)
    gate = jnp.sum(jnp.where(lanes % num_experts == me, packed, 0.0), axis=-1, keepdims=True)
    u_val = jnp.dot(x_val, wg_ref[0], preferred_element_type=jnp.float32)
    v_val = jnp.dot(x_val, wu_ref[0], preferred_element_type=jnp.float32)
    z_val = (u_val * jax.nn.sigmoid(u_val) * v_val).astype(jnp.bfloat16)
    y_val = jnp.dot(z_val, wd_ref[0], preferred_element_type=jnp.float32).astype(jnp.bfloat16)
    y_ref[...] = gate * y_val.astype(jnp.float32)


def expert_mlp(rows_in, w_gate, w_up, w_down, num_experts):
    rows, width = rows_in.shape
    d_ff, d_model = w_down.shape[1:]
    tile = 256

    def fixed(arr):
        return pl.BlockSpec(arr.shape, lambda i: (0, 0, 0), pipeline_mode=pl.Buffered(1))

    return pl.pallas_call(
        functools.partial(expert_kernel, num_experts),
        grid=(rows // tile,),
        in_specs=[pl.BlockSpec((tile, width), lambda i: (i, 0)), fixed(w_gate), fixed(w_up), fixed(w_down)],
        out_specs=pl.BlockSpec((tile, d_model), lambda i: (i, 0)),
        out_shape=jax.ShapeDtypeStruct((rows, d_model), jnp.float32),
        compiler_params=pltpu.CompilerParams(dimension_semantics=("arbitrary",), vmem_limit_bytes=52 * MIB),
        cost_estimate=pl.CostEstimate(flops=6 * rows * d_model * d_ff, bytes_accessed=6 * d_model * d_ff, transcendentals=0),
    )(rows_in, w_gate, w_up, w_down)


def solution(mesh):
    def local_step(tokens, k_cache, v_cache, positions, expert_one, expert_two, eligible, ln1_gain, ln1_bias, w_query, b_query, w_key, b_key, w_value, b_value, w_out, b_out, ln2_gain, ln2_bias, w_router, w_gate, w_up, w_down):
        rows, d_model = tokens.shape
        _, seq_len, kv_heads, head_dim = k_cache.shape
        num_heads = w_query.shape[1] // head_dim
        num_experts = w_router.shape[1]
        cos_tab, sin_tab = rope_tables(positions, head_dim)
        q_flat, k_flat, v_flat = qkv_project(tokens, ln1_gain, ln1_bias, cos_tab, sin_tab, w_query, w_key, w_value, b_query, b_key, b_value, head_dim)
        key_new = k_flat.reshape(rows, kv_heads, head_dim)
        value_new = v_flat.reshape(rows, kv_heads, head_dim)
        attn = attend(positions, q_flat.reshape(rows, num_heads, head_dim), key_new, value_new, k_cache, v_cache)
        x_mid, send = post_attention(attn.reshape(rows, num_heads * head_dim), w_out, b_out, tokens, ln2_gain, ln2_bias, w_router, expert_one, expert_two, eligible)
        chunk = rows // CHUNKS
        arrived = [lax.all_gather(send[c * chunk:(c + 1) * chunk], 'ep', axis=0, tiled=True) for c in range(CHUNKS)]
        outs = []
        for c in range(CHUNKS):
            partial = expert_mlp(arrived[c], w_gate, w_up, w_down, num_experts)
            y_sum = lax.psum_scatter(partial, 'ep', scatter_dimension=0, tiled=True)
            outs.append((x_mid[c * chunk:(c + 1) * chunk].astype(jnp.float32) + y_sum).astype(jnp.bfloat16))
        tokens_out = jnp.concatenate(outs, axis=0)
        return tokens_out, key_new, value_new

    row_spec = P('ep', None)
    cache_spec = P('ep', None, None, None)
    vec_spec = P('ep')
    rep_one = P(None)
    rep_two = P(None, None)
    expert_spec = P('ep', None, None)
    in_specs = (row_spec, cache_spec, cache_spec, vec_spec, vec_spec, vec_spec, row_spec, rep_one, rep_one, rep_two, rep_one, rep_two, rep_one, rep_two, rep_one, rep_two, rep_one, rep_one, rep_one, rep_two, expert_spec, expert_spec, expert_spec)
    out_specs = (row_spec, expert_spec, expert_spec)
    return jax.shard_map(local_step, mesh=mesh, in_specs=in_specs, out_specs=out_specs, check_vma=False)
```

```python
import functools

import jax
import jax.numpy as jnp
from jax import lax
from jax.experimental import pallas as pl
from jax.experimental.pallas import tpu as pltpu
from jax.sharding import PartitionSpec as P

ROPE_BASE = 10000.0
LN_EPS = 1e-5
MIB = 1024 * 1024


def layer_norm_rows(x, gain, bias):
    mean_val = jnp.mean(x, axis=-1, keepdims=True)
    centered = x - mean_val
    var_val = jnp.mean(centered * centered, axis=-1, keepdims=True)
    return centered * lax.rsqrt(var_val + LN_EPS) * gain + bias


def rope_tables(positions, head_dim):
    half_dim = head_dim // 2
    inv_freq = ROPE_BASE ** (jnp.arange(half_dim, dtype=jnp.float32) * (-2.0 / head_dim))
    angles = positions.astype(jnp.float32)[:, None] * inv_freq[None, :]
    cos_val, sin_val = jnp.cos(angles), jnp.sin(angles)
    return jnp.concatenate([cos_val, cos_val], axis=-1), jnp.concatenate([-sin_val, sin_val], axis=-1)


def qkv_kernel(head_dim, q_steps, kv_steps, tok_ref, gain_ref, bias_ref, cos_ref, sin_ref, wq_ref, wk_ref, wv_ref, bq_ref, bk_ref, bv_ref, q_ref, k_ref, v_ref, h_ref):
    step = pl.program_id(0)

    @pl.when(step == 0)
    def _():
        x = tok_ref[...].astype(jnp.float32)
        h_ref[...] = layer_norm_rows(x, gain_ref[...].astype(jnp.float32), bias_ref[...].astype(jnp.float32)).astype(jnp.bfloat16)

    def project(w_ref, b_ref):
        return jnp.dot(h_ref[...], w_ref[...], preferred_element_type=jnp.float32) + b_ref[...].astype(jnp.float32)

    def rotated(y, out_ref):
        for head in range(y.shape[1] // head_dim):
            cols = slice(head * head_dim, (head + 1) * head_dim)
            part = y[:, cols]
            turned = pltpu.roll(part, head_dim // 2, 1)
            out_ref[:, cols] = (part * cos_ref[...] + turned * sin_ref[...]).astype(jnp.bfloat16)

    @pl.when(step < q_steps)
    def _():
        rotated(project(wq_ref, bq_ref), q_ref)

    @pl.when((step >= q_steps) & (step < q_steps + kv_steps))
    def _():
        rotated(project(wk_ref, bk_ref), k_ref)

    @pl.when(step >= q_steps + kv_steps)
    def _():
        v_ref[...] = project(wv_ref, bv_ref).astype(jnp.bfloat16)


def qkv_project(tokens, gain, bias, cos_tab, sin_tab, w_query, w_key, w_value, b_query, b_key, b_value, head_dim):
    rows, d_model = tokens.shape
    q_dim, kv_dim = w_query.shape[1], w_key.shape[1]
    block = 512
    q_steps, kv_steps = q_dim // block, kv_dim // block

    def q_idx(i):
        return (0, jnp.minimum(i, q_steps - 1))

    def k_idx(i):
        return (0, jnp.clip(i - q_steps, 0, kv_steps - 1))

    def v_idx(i):
        return (0, jnp.clip(i - q_steps - kv_steps, 0, kv_steps - 1))

    def whole(arr):
        return pl.BlockSpec(arr.shape, lambda i: (0,) * arr.ndim)

    gain, bias = gain[None, :], bias[None, :]
    return pl.pallas_call(
        functools.partial(qkv_kernel, head_dim, q_steps, kv_steps),
        grid=(q_steps + 2 * kv_steps,),
        in_specs=[
            whole(tokens), whole(gain), whole(bias), whole(cos_tab), whole(sin_tab),
            pl.BlockSpec((d_model, block), q_idx), pl.BlockSpec((d_model, block), k_idx), pl.BlockSpec((d_model, block), v_idx),
            pl.BlockSpec((1, block), q_idx), pl.BlockSpec((1, block), k_idx), pl.BlockSpec((1, block), v_idx),
        ],
        out_specs=[pl.BlockSpec((rows, block), q_idx), pl.BlockSpec((rows, block), k_idx), pl.BlockSpec((rows, block), v_idx)],
        out_shape=[jax.ShapeDtypeStruct((rows, q_dim), jnp.bfloat16), jax.ShapeDtypeStruct((rows, kv_dim), jnp.bfloat16), jax.ShapeDtypeStruct((rows, kv_dim), jnp.bfloat16)],
        scratch_shapes=[pltpu.VMEM((rows, d_model), jnp.bfloat16)],
        compiler_params=pltpu.CompilerParams(dimension_semantics=("arbitrary",), vmem_limit_bytes=40 * MIB),
        cost_estimate=pl.CostEstimate(flops=2 * rows * d_model * (q_dim + 2 * kv_dim), bytes_accessed=2 * d_model * (q_dim + 2 * kv_dim), transcendentals=0),
    )(tokens, gain, bias, cos_tab, sin_tab, w_query, w_key, w_value, b_query[None, :], b_key[None, :], b_value[None, :])


def attend_kernel(batch, ahead, kv_heads, group_size, pos_ref, q_ref, kn_ref, vn_ref, k_hbm, v_hbm, out_ref, k_buf, v_buf, where_ref, k_sem, v_sem):
    tok_count, seq_len = k_hbm.shape[0], k_hbm.shape[1]
    num_heads, head_dim = q_ref.shape[1], q_ref.shape[2]
    rounds = tok_count // batch
    slots = ahead + 1
    cols = seq_len * kv_heads
    v_buf[...] = jnp.zeros_like(v_buf)
    col_ids = lax.broadcasted_iota(jnp.int32, (num_heads, cols), 1)
    head_ids = lax.broadcasted_iota(jnp.int32, (num_heads, cols), 0)
    where_ref[...] = jnp.where(col_ids % kv_heads == head_ids // group_size, col_ids // kv_heads, seq_len)

    def copies(turn, lane):
        tok = turn * batch + lane
        slot = lax.rem(turn, slots)
        count = ((pos_ref[tok] + 7) // 8) * 8
        k_copy = pltpu.make_async_copy(k_hbm.at[tok, pl.ds(0, count)], k_buf.at[slot, lane, pl.ds(0, count)], k_sem.at[slot])
        v_copy = pltpu.make_async_copy(v_hbm.at[tok, pl.ds(0, count)], v_buf.at[slot, lane, pl.ds(0, count)], v_sem.at[slot])
        return k_copy, v_copy

    def fetch(turn):
        for lane in range(batch):
            for copy in copies(turn, lane):
                copy.start()

    for turn in range(ahead):
        fetch(turn)

    scale = head_dim ** -0.5

    def one_round(turn, carry):
        @pl.when(turn + ahead < rounds)
        def _():
            fetch(turn + ahead)

        slot = lax.rem(turn, slots)
        for lane in range(batch):
            for copy in copies(turn, lane):
                copy.wait()
        for lane in range(batch):
            tok = turn * batch + lane
            pos = pos_ref[tok]
            k_buf[slot, lane, pos] = kn_ref[tok]
            v_buf[slot, lane, pos] = vn_ref[tok]
        for lane in range(batch):
            tok = turn * batch + lane
            pos = pos_ref[tok]
            k_all = k_buf[slot, lane].reshape(cols, head_dim)
            v_all = v_buf[slot, lane].reshape(cols, head_dim)
            s_val = lax.dot_general(q_ref[tok], k_all, (((1,), (1,)), ((), ())), preferred_element_type=jnp.float32) * scale
            s_val = jnp.where(where_ref[...] <= pos, s_val, -jnp.inf)
            e_val = jnp.exp(s_val - jnp.max(s_val, axis=-1, keepdims=True))
            p_val = (e_val * (1.0 / jnp.sum(e_val, axis=-1, keepdims=True))).astype(jnp.bfloat16)
            out_ref[tok] = jnp.dot(p_val, v_all, preferred_element_type=jnp.float32).astype(jnp.bfloat16)
        return carry

    lax.fori_loop(0, rounds, one_round, 0)


def attend(positions, q_heads, key_new, value_new, k_cache, v_cache):
    tok_count, seq_len, kv_heads, head_dim = k_cache.shape
    num_heads = q_heads.shape[1]
    batch, ahead = 4, 3
    buf = pltpu.VMEM((ahead + 1, batch, seq_len, kv_heads, head_dim), jnp.bfloat16)
    vmem = pl.BlockSpec(memory_space=pltpu.VMEM)
    return pl.pallas_call(
        functools.partial(attend_kernel, batch, ahead, kv_heads, num_heads // kv_heads),
        in_specs=[pl.BlockSpec(memory_space=pltpu.SMEM), vmem, vmem, vmem, pl.BlockSpec(memory_space=pltpu.HBM), pl.BlockSpec(memory_space=pltpu.HBM)],
        out_specs=vmem,
        out_shape=jax.ShapeDtypeStruct(q_heads.shape, jnp.bfloat16),
        scratch_shapes=[buf, buf, pltpu.VMEM((num_heads, seq_len * kv_heads), jnp.int32), pltpu.SemaphoreType.DMA((ahead + 1,)), pltpu.SemaphoreType.DMA((ahead + 1,))],
        compiler_params=pltpu.CompilerParams(vmem_limit_bytes=32 * MIB),
        cost_estimate=pl.CostEstimate(flops=4 * tok_count * num_heads * seq_len * kv_heads * head_dim, bytes_accessed=4 * k_cache.size, transcendentals=0),
    )(positions, q_heads, key_new, value_new, k_cache, v_cache)


def post_kernel(num_experts, steps, attn_ref, wo_ref, bo_ref, tok_ref, gain_ref, bias_ref, wr_ref, one_ref, two_ref, elig_ref, x_ref, send_ref, acc_ref):
    step = pl.program_id(0)
    block = wo_ref.shape[1]
    cols = pl.ds(pl.multiple_of(step * block, block), block)
    mixed = jnp.dot(attn_ref[...], wo_ref[...], preferred_element_type=jnp.float32)
    x_mid = (tok_ref[...].astype(jnp.float32) + mixed + bo_ref[...].astype(jnp.float32)).astype(jnp.bfloat16)
    x_ref[...] = x_mid
    acc_ref[:, cols] = x_mid

    @pl.when(step == steps - 1)
    def _():
        h_two = layer_norm_rows(acc_ref[...].astype(jnp.float32), gain_ref[...].astype(jnp.float32), bias_ref[...].astype(jnp.float32)).astype(jnp.bfloat16)
        logits = jnp.dot(h_two, wr_ref[...], preferred_element_type=jnp.float32)
        rows, width = logits.shape
        lanes = lax.broadcasted_iota(jnp.int32, (rows, width), 1)
        hit_one = lanes == one_ref[...]
        hit_two = lanes == two_ref[...]
        keep_one = elig_ref[...] == 1
        keep_two = keep_one & jnp.logical_not(hit_one)

        def gate(keep, hit):
            masked = jnp.where(keep, logits, -jnp.inf)
            e_val = jnp.exp(masked - jnp.max(masked, axis=-1, keepdims=True))
            return jnp.sum(jnp.where(hit, e_val, 0.0), axis=-1, keepdims=True) / jnp.sum(e_val, axis=-1, keepdims=True)

        gates = jnp.where(hit_one, gate(keep_one, hit_one), 0.0) + jnp.where(hit_two, gate(keep_two, hit_two), 0.0)
        high = gates.astype(jnp.bfloat16).astype(jnp.float32)
        rest = gates - high
        mid = rest.astype(jnp.bfloat16).astype(jnp.float32)
        packed = high + pltpu.roll(mid, num_experts, 1) + pltpu.roll(rest - mid, 2 * num_experts, 1)
        d_model = h_two.shape[1]
        send_ref[:, :d_model] = h_two
        send_ref[:, d_model:] = packed.astype(jnp.bfloat16)


def post_attention(attn, w_out, b_out, tokens, gain, bias, w_router, expert_one, expert_two, eligible):
    rows, d_model = tokens.shape
    num_experts = w_router.shape[1]
    width = 128
    block = 512
    steps = d_model // block
    w_router = jnp.pad(w_router, ((0, 0), (0, width - num_experts)))
    eligible = jnp.pad(eligible, ((0, 0), (0, width - num_experts)))
    one, two = expert_one[:, None], expert_two[:, None]
    gain, bias = gain[None, :], bias[None, :]

    def whole(arr):
        return pl.BlockSpec(arr.shape, lambda i: (0,) * arr.ndim)

    def col(i):
        return (0, i)

    return pl.pallas_call(
        functools.partial(post_kernel, num_experts, steps),
        grid=(steps,),
        in_specs=[
            whole(attn), pl.BlockSpec((attn.shape[1], block), col), pl.BlockSpec((1, block), col), pl.BlockSpec((rows, block), col),
            whole(gain), whole(bias), whole(w_router), whole(one), whole(two), whole(eligible),
        ],
        out_specs=[pl.BlockSpec((rows, block), col), pl.BlockSpec((rows, d_model + width), lambda i: (0, 0))],
        out_shape=[jax.ShapeDtypeStruct((rows, d_model), jnp.bfloat16), jax.ShapeDtypeStruct((rows, d_model + width), jnp.bfloat16)],
        scratch_shapes=[pltpu.VMEM((rows, d_model), jnp.bfloat16)],
        compiler_params=pltpu.CompilerParams(dimension_semantics=("arbitrary",), vmem_limit_bytes=48 * MIB),
        cost_estimate=pl.CostEstimate(flops=2 * rows * d_model * d_model, bytes_accessed=2 * d_model * d_model, transcendentals=0),
    )(attn, w_out, b_out[None, :], tokens, gain, bias, w_router, one, two, eligible)


STEP_ROWS = 16
DIMS = 3


def moe_kernel(num_experts, h_ref, xm_ref, wg_hbm, wu_hbm, wd_hbm, out_ref, all_ref, wg_ref, wu_ref, wd_ref, x_buf, y_buf, mate_buf, keep_refs, send_refs, recv_refs, w_sem, x_sem, own_sem, gs_sem, gr_sem, ms_sem, mr_sem, mate_s, mate_r, mate_free, red_s, red_r, red_free):
    me = lax.axis_index('ep')
    core = lax.rem(me, 2)
    chip = me // 2
    mate = chip * 2 + 1 - core
    rows, d_model = xm_ref.shape
    width = h_ref.shape[1]
    third = width // 3
    chunks = rows // STEP_ROWS
    logical = pl.DeviceIdType.MESH

    def bit(dim):
        return (chip // (1 << dim)) % 2

    def across(who, dim):
        return who + (1 - 2 * ((who // (1 << dim)) % 2)) * (1 << dim)

    def device_of(who):
        return who * 2 + core

    peers = [device_of(across(chip, dim)) for dim in range(DIMS)]

    weights = [pltpu.make_async_copy(src.at[0], dst, w_sem.at[n]) for n, (src, dst) in enumerate(((wg_hbm, wg_ref), (wu_hbm, wu_ref), (wd_hbm, wd_ref)))]
    for copy in weights:
        copy.start()
    own = pltpu.make_async_copy(h_ref, all_ref.at[me], own_sem)
    own.start()

    barrier = pltpu.get_barrier_semaphore()
    for peer in peers + [mate]:
        pl.semaphore_signal(barrier, inc=1, device_id=(peer,), device_id_type=logical)
    pl.semaphore_wait(barrier, DIMS + 1)

    def piece(owner, part, mine):
        cols = pl.ds(part * third, third)
        src = h_ref.at[:, cols] if mine else all_ref.at[owner, :, cols]
        return src, all_ref.at[owner, :, cols]

    def spread(owner, part, slot, peer, mine):
        src, dst = piece(owner, part, mine)
        return pltpu.make_async_remote_copy(src, dst, gs_sem.at[part, slot], gr_sem.at[part, slot], device_id=(peer,), device_id_type=logical)

    def share(owner, part, slot, mine):
        src, dst = piece(owner, part, mine)
        return pltpu.make_async_remote_copy(src, dst, ms_sem.at[part, slot], mr_sem.at[part, slot], device_id=(mate,), device_id_type=logical)

    started = []
    for part in range(3):
        copy = share(me, part, 0, True)
        copy.start()
        started.append(copy)
    held = [[chip] for _ in range(3)]
    base = 0
    for step in range(DIMS):
        wave = []
        for part in range(3):
            dim = (part + step) % 3
            for n, who in enumerate(held[part]):
                copy = spread(device_of(who), part, base + n, peers[dim], n == 0)
                copy.start()
                wave.append(copy)
                started.append(copy)
        for part in range(3):
            dim = (part + step) % 3
            count = len(held[part])
            fresh = [across(who, dim) for who in held[part]]
            for n, who in enumerate(fresh):
                wave[part * count + n].wait_recv()
                copy = share(device_of(who), part, 1 + base + n, False)
                copy.start()
                started.append(copy)
            held[part] = held[part] + fresh
        base += 1 << step
    for copy in weights:
        copy.wait()
    own.wait()
    for part in range(3):
        for slot in range(8):
            share(me, part, slot, True).wait_recv()
    for copy in started:
        copy.wait_send()

    spans = []
    at = 0
    for ref in keep_refs[:3]:
        spans.append((at, ref.shape[-1]))
        at += ref.shape[-1]

    def x_copy(c):
        return pltpu.make_async_copy(all_ref.at[:, pl.ds(pl.multiple_of(c * STEP_ROWS, STEP_ROWS), STEP_ROWS)], x_buf, x_sem)

    def mate_copy(c):
        slot = lax.rem(c, 2)
        return pltpu.make_async_remote_copy(y_buf.at[slot, :, 1 - core], mate_buf.at[slot], mate_s.at[slot], mate_r.at[slot], device_id=(mate,), device_id_type=logical)

    def red_copy(c, level, part):
        slot = lax.rem(c, 2)
        n = level * 3 + part
        return pltpu.make_async_remote_copy(send_refs[n].at[slot], recv_refs[n].at[slot], red_s.at[n, slot], red_r.at[n, slot], device_id=(peers[(part + level) % 3],), device_id_type=logical)

    def experts(c):
        slot = lax.rem(c, 2)
        x_copy(c).wait()

        @pl.when(c >= 2)
        def _():
            mate_copy(c - 2).wait_send()

        x_all = x_buf[...].reshape(num_experts * STEP_ROWS, width)
        packed = x_all[:, d_model:].astype(jnp.float32)
        lanes = lax.broadcasted_iota(jnp.int32, packed.shape, 1)
        gate = jnp.sum(jnp.where(lanes % num_experts == me, packed, 0.0), axis=-1, keepdims=True)
        x_val = x_all[:, :d_model]
        flat = (((1,), (1,)), ((), ()))
        u_val = lax.dot_general(x_val, wg_ref[...], flat, preferred_element_type=jnp.float32)
        v_val = lax.dot_general(x_val, wu_ref[...], flat, preferred_element_type=jnp.float32)
        z_val = (u_val * jax.nn.sigmoid(u_val) * v_val).astype(jnp.bfloat16)
        block = 1024
        for n in range(d_model // block):
            cols = slice(n * block, (n + 1) * block)
            y_val = jnp.dot(z_val, wd_ref[:, cols], preferred_element_type=jnp.float32).astype(jnp.bfloat16)
            y_buf[slot, :, :, :, cols] = (gate * y_val.astype(jnp.float32)).reshape(num_experts // 2, 2, STEP_ROWS, block)

        @pl.when(c >= 2)
        def _():
            pl.semaphore_wait(mate_free, 1)

        mate_copy(c).start()

        @pl.when(c + 1 < chunks)
        def _():
            x_copy(c + 1).start()

    def give(c, level):
        for part in range(3):
            @pl.when(c >= 2)
            def _():
                pl.semaphore_wait(red_free.at[level * 3 + part], 1)

            red_copy(c, level, part).start()

    def drained(c, level):
        @pl.when(c >= 2)
        def _():
            for part in range(3):
                red_copy(c - 2, level, part).wait_send()

    def first(c):
        slot = lax.rem(c, 2)
        mate_copy(c).wait_recv()
        drained(c, 0)
        for part in range(3):
            lo, size = spans[part]
            cols = slice(lo, lo + size)
            dims = [(part + k) % 3 for k in range(3)]
            for n in range(4):
                rest = (n % 2) * (1 << dims[1]) + (n // 2) * (1 << dims[2])
                for side, refs in ((bit(dims[0]), keep_refs), (1 - bit(dims[0]), send_refs)):
                    who = rest + side * (1 << dims[0])
                    refs[part][slot, n] = y_buf[slot, who, core, :, cols] + mate_buf[slot, who, :, cols]

        @pl.when(c + 2 < chunks)
        def _():
            pl.semaphore_signal(mate_free, inc=1, device_id=(mate,), device_id_type=logical)

        give(c, 0)

    def later(c, level):
        slot = lax.rem(c, 2)
        old, new = (level - 1) * 3, level * 3
        drained(c, level)
        for part in range(3):
            red_copy(c, level - 1, part).wait_recv()
            dim = (part + level) % 3
            for n in range(1 << (2 - level)):
                for side, refs in ((bit(dim), keep_refs), (1 - bit(dim), send_refs)):
                    at = n * 2 + side
                    refs[new + part][slot, n] = keep_refs[old + part][slot, at] + recv_refs[old + part][slot, at]

            @pl.when(c + 2 < chunks)
            def _():
                pl.semaphore_signal(red_free.at[old + part], inc=1, device_id=(peers[(part + level - 1) % 3],), device_id_type=logical)

        give(c, level)

    def last(c):
        slot = lax.rem(c, 2)
        here = pl.ds(pl.multiple_of(c * STEP_ROWS, STEP_ROWS), STEP_ROWS)
        for part in range(3):
            red_copy(c, 2, part).wait_recv()
            lo, size = spans[part]
            cols = slice(lo, lo + size)
            y_sum = keep_refs[6 + part][slot, 0] + recv_refs[6 + part][slot, 0]
            out_ref[here, cols] = (xm_ref[here, cols].astype(jnp.float32) + y_sum).astype(jnp.bfloat16)

            @pl.when(c + 2 < chunks)
            def _():
                pl.semaphore_signal(red_free.at[6 + part], inc=1, device_id=(peers[(part + 2) % 3],), device_id_type=logical)

    x_copy(0).start()

    def turn(i, carry):
        @pl.when(i < chunks)
        def _():
            experts(i)

        @pl.when((i >= 1) & (i - 1 < chunks))
        def _():
            first(i - 1)

        @pl.when(i >= 4)
        def _():
            last(i - 4)

        @pl.when((i >= 3) & (i - 3 < chunks))
        def _():
            later(i - 3, 2)

        @pl.when((i >= 2) & (i - 2 < chunks))
        def _():
            later(i - 2, 1)

        return carry

    lax.fori_loop(0, chunks + 4, turn, 0)
    for c in (chunks - 2, chunks - 1):
        mate_copy(c).wait_send()
        for level in range(3):
            for part in range(3):
                red_copy(c, level, part).wait_send()


def moe_layer(h_rows, x_mid, w_gate, w_up, w_down, num_experts):
    rows, width = h_rows.shape
    d_ff, d_model = w_down.shape[1:]
    unit = d_model // 128
    sizes = [128 * (unit // 3 + (1 if part < unit % 3 else 0)) for part in range(3)]
    chips = num_experts // 2
    f32 = jnp.float32

    def level_bufs():
        return [pltpu.VMEM((2, chips >> (level + 1), STEP_ROWS, sizes[part]), f32) for level in range(3) for part in range(3)]

    vmem = pl.BlockSpec(memory_space=pltpu.VMEM)
    hbm = pl.BlockSpec(memory_space=pltpu.HBM)
    dma = pltpu.SemaphoreType.DMA
    regular = pltpu.SemaphoreType.REGULAR
    out, _ = pl.pallas_call(
        functools.partial(moe_kernel, num_experts),
        in_specs=[vmem, vmem, hbm, hbm, hbm],
        out_specs=[vmem, hbm],
        out_shape=[jax.ShapeDtypeStruct((rows, d_model), jnp.bfloat16), jax.ShapeDtypeStruct((num_experts, rows, width), jnp.bfloat16)],
        scratch_shapes=[
            pltpu.VMEM((d_ff, d_model), jnp.bfloat16), pltpu.VMEM((d_ff, d_model), jnp.bfloat16), pltpu.VMEM((d_ff, d_model), jnp.bfloat16),
            pltpu.VMEM((num_experts, STEP_ROWS, width), jnp.bfloat16),
            pltpu.VMEM((2, chips, 2, STEP_ROWS, d_model), f32),
            pltpu.VMEM((2, chips, STEP_ROWS, d_model), f32),
            level_bufs(), level_bufs(), level_bufs(),
            dma((3,)), dma, dma, dma((3, 7)), dma((3, 7)), dma((3, 8)), dma((3, 8)),
            dma((2,)), dma((2,)), regular, dma((9, 2)), dma((9, 2)), regular((9,)),
        ],
        compiler_params=pltpu.CompilerParams(collective_id=0, has_side_effects=True, vmem_limit_bytes=67043328),
        cost_estimate=pl.CostEstimate(flops=6 * rows * num_experts * d_model * d_ff, bytes_accessed=6 * d_model * d_ff, transcendentals=0),
    )(h_rows, x_mid, jnp.swapaxes(w_gate, 1, 2), jnp.swapaxes(w_up, 1, 2), w_down)
    return out


def solution(mesh):
    def local_step(tokens, k_cache, v_cache, positions, expert_one, expert_two, eligible, ln1_gain, ln1_bias, w_query, b_query, w_key, b_key, w_value, b_value, w_out, b_out, ln2_gain, ln2_bias, w_router, w_gate, w_up, w_down):
        rows, d_model = tokens.shape
        _, seq_len, kv_heads, head_dim = k_cache.shape
        num_heads = w_query.shape[1] // head_dim
        num_experts = w_router.shape[1]
        cos_tab, sin_tab = rope_tables(positions, head_dim)
        q_flat, k_flat, v_flat = qkv_project(tokens, ln1_gain, ln1_bias, cos_tab, sin_tab, w_query, w_key, w_value, b_query, b_key, b_value, head_dim)
        key_new = k_flat.reshape(rows, kv_heads, head_dim)
        value_new = v_flat.reshape(rows, kv_heads, head_dim)
        attn = attend(positions, q_flat.reshape(rows, num_heads, head_dim), key_new, value_new, k_cache, v_cache)
        x_mid, send = post_attention(attn.reshape(rows, num_heads * head_dim), w_out, b_out, tokens, ln2_gain, ln2_bias, w_router, expert_one, expert_two, eligible)
        tokens_out = moe_layer(send, x_mid, w_gate, w_up, w_down, num_experts)
        return tokens_out, key_new, value_new

    row_spec = P('ep', None)
    cache_spec = P('ep', None, None, None)
    vec_spec = P('ep')
    rep_one = P(None)
    rep_two = P(None, None)
    expert_spec = P('ep', None, None)
    in_specs = (row_spec, cache_spec, cache_spec, vec_spec, vec_spec, vec_spec, row_spec, rep_one, rep_one, rep_two, rep_one, rep_two, rep_one, rep_two, rep_one, rep_two, rep_one, rep_one, rep_one, rep_two, expert_spec, expert_spec, expert_spec)
    out_specs = (row_spec, expert_spec, expert_spec)
    return jax.shard_map(local_step, mesh=mesh, in_specs=in_specs, out_specs=out_specs, check_vma=False)
```

```python
import functools

import jax
import jax.numpy as jnp
from jax import lax
from jax.experimental import pallas as pl
from jax.experimental.pallas import tpu as pltpu
from jax.sharding import PartitionSpec as P

ROPE_BASE = 10000.0
LN_EPS = 1e-5
MIB = 1024 * 1024


def layer_norm_rows(x, gain, bias):
    mean_val = jnp.mean(x, axis=-1, keepdims=True)
    centered = x - mean_val
    var_val = jnp.mean(centered * centered, axis=-1, keepdims=True)
    return centered * lax.rsqrt(var_val + LN_EPS) * gain + bias


def rope_tables(positions, head_dim):
    half_dim = head_dim // 2
    inv_freq = ROPE_BASE ** (jnp.arange(half_dim, dtype=jnp.float32) * (-2.0 / head_dim))
    angles = positions.astype(jnp.float32)[:, None] * inv_freq[None, :]
    cos_val, sin_val = jnp.cos(angles), jnp.sin(angles)
    return jnp.concatenate([cos_val, cos_val], axis=-1), jnp.concatenate([-sin_val, sin_val], axis=-1)


def qkv_kernel(head_dim, q_steps, kv_steps, tok_ref, vec_ref, cos_ref, sin_ref, wq_ref, wk_ref, wv_ref, bq_ref, bkv_ref, q_ref, k_ref, v_ref, h_ref):
    step = pl.program_id(0)

    @pl.when(step == 0)
    def _():
        x = tok_ref[...].astype(jnp.float32)
        h_ref[...] = layer_norm_rows(x, vec_ref[0:1, :], vec_ref[1:2, :]).astype(jnp.bfloat16)

    def project(w_ref, b_row):
        return jnp.dot(h_ref[...], w_ref[...], preferred_element_type=jnp.float32) + b_row

    def rotated(y, out_ref):
        for head in range(y.shape[1] // head_dim):
            cols = slice(head * head_dim, (head + 1) * head_dim)
            part = y[:, cols]
            turned = pltpu.roll(part, head_dim // 2, 1)
            out_ref[:, cols] = (part * cos_ref[...] + turned * sin_ref[...]).astype(jnp.bfloat16)

    @pl.when(step < q_steps)
    def _():
        rotated(project(wq_ref, bq_ref[2:3, :]), q_ref)

    @pl.when((step >= q_steps) & (step < q_steps + kv_steps))
    def _():
        rotated(project(wk_ref, bkv_ref[3:4, :]), k_ref)

    @pl.when(step >= q_steps + kv_steps)
    def _():
        v_ref[...] = project(wv_ref, bkv_ref[3:4, :]).astype(jnp.bfloat16)


def qkv_project(tokens, vecs, cos_tab, sin_tab, w_query, w_key, w_value, head_dim):
    rows, d_model = tokens.shape
    q_dim, kv_dim = w_query.shape[1], w_key.shape[1]
    block = 512
    q_steps, kv_steps = q_dim // block, kv_dim // block

    def q_idx(i):
        return (0, jnp.minimum(i, q_steps - 1))

    def k_idx(i):
        return (0, jnp.clip(i - q_steps, 0, kv_steps - 1))

    def v_idx(i):
        return (0, jnp.clip(i - q_steps - kv_steps, 0, kv_steps - 1))

    def whole(arr):
        return pl.BlockSpec(arr.shape, lambda i: (0,) * arr.ndim)

    def kv_idx(i):
        return (0, jnp.clip(i - q_steps, 0, 2 * kv_steps - 1))

    return pl.pallas_call(
        functools.partial(qkv_kernel, head_dim, q_steps, kv_steps),
        grid=(q_steps + 2 * kv_steps,),
        in_specs=[
            whole(tokens), whole(vecs), whole(cos_tab), whole(sin_tab),
            pl.BlockSpec((d_model, block), q_idx), pl.BlockSpec((d_model, block), k_idx), pl.BlockSpec((d_model, block), v_idx),
            pl.BlockSpec((vecs.shape[0], block), q_idx), pl.BlockSpec((vecs.shape[0], block), kv_idx),
        ],
        out_specs=[pl.BlockSpec((rows, block), q_idx), pl.BlockSpec((rows, block), k_idx), pl.BlockSpec((rows, block), v_idx)],
        out_shape=[jax.ShapeDtypeStruct((rows, q_dim), jnp.bfloat16), jax.ShapeDtypeStruct((rows, kv_dim), jnp.bfloat16), jax.ShapeDtypeStruct((rows, kv_dim), jnp.bfloat16)],
        scratch_shapes=[pltpu.VMEM((rows, d_model), jnp.bfloat16)],
        compiler_params=pltpu.CompilerParams(dimension_semantics=("arbitrary",), vmem_limit_bytes=62 * MIB),
        cost_estimate=pl.CostEstimate(flops=2 * rows * d_model * (q_dim + 2 * kv_dim), bytes_accessed=2 * d_model * (q_dim + 2 * kv_dim), transcendentals=0),
    )(tokens, vecs, cos_tab, sin_tab, w_query, w_key, w_value, vecs, vecs)


def attend_kernel(batch, ahead, kv_heads, group_size, pos_ref, q_ref, kn_ref, vn_ref, k_hbm, v_hbm, out_ref, k_buf, v_buf, where_ref, k_sem, v_sem):
    tok_count, seq_len = k_hbm.shape[0], k_hbm.shape[1]
    num_heads, head_dim = q_ref.shape[1], q_ref.shape[2]
    rounds = tok_count // batch
    slots = ahead + 1
    cols = seq_len * kv_heads
    v_buf[...] = jnp.zeros_like(v_buf)
    col_ids = lax.broadcasted_iota(jnp.int32, (num_heads, cols), 1)
    head_ids = lax.broadcasted_iota(jnp.int32, (num_heads, cols), 0)
    where_ref[...] = jnp.where(col_ids % kv_heads == head_ids // group_size, col_ids // kv_heads, seq_len)

    half = seq_len // 2

    def copies(turn, lane, part):
        tok = turn * batch + lane
        slot = lax.rem(turn, slots)
        rows = pl.ds(part * half, half)
        k_copy = pltpu.make_async_copy(k_hbm.at[tok, rows], k_buf.at[slot, lane, rows], k_sem.at[slot])
        v_copy = pltpu.make_async_copy(v_hbm.at[tok, rows], v_buf.at[slot, lane, rows], v_sem.at[slot])
        return k_copy, v_copy

    def each(turn, act):
        for lane in range(batch):
            for copy in copies(turn, lane, 0):
                act(copy)

            @pl.when(pos_ref[turn * batch + lane] > half)
            def _():
                for copy in copies(turn, lane, 1):
                    act(copy)

    def fetch(turn):
        each(turn, lambda copy: copy.start())

    for turn in range(ahead):
        fetch(turn)

    scale = head_dim ** -0.5

    def one_round(turn, carry):
        @pl.when(turn + ahead < rounds)
        def _():
            fetch(turn + ahead)

        slot = lax.rem(turn, slots)
        each(turn, lambda copy: copy.wait())
        for lane in range(batch):
            tok = turn * batch + lane
            pos = pos_ref[tok]
            k_buf[slot, lane, pos] = kn_ref[tok]
            v_buf[slot, lane, pos] = vn_ref[tok]
        for lane in range(batch):
            tok = turn * batch + lane
            pos = pos_ref[tok]
            k_all = k_buf[slot, lane].reshape(cols, head_dim)
            v_all = v_buf[slot, lane].reshape(cols, head_dim)
            s_val = lax.dot_general(q_ref[tok], k_all, (((1,), (1,)), ((), ())), preferred_element_type=jnp.float32) * scale
            s_val = jnp.where(where_ref[...] <= pos, s_val, -jnp.inf)
            e_val = jnp.exp(s_val - jnp.max(s_val, axis=-1, keepdims=True))
            p_val = (e_val * (1.0 / jnp.sum(e_val, axis=-1, keepdims=True))).astype(jnp.bfloat16)
            out_ref[tok] = jnp.dot(p_val, v_all, preferred_element_type=jnp.float32).astype(jnp.bfloat16)
        return carry

    lax.fori_loop(0, rounds, one_round, 0)


def attend(positions, q_heads, key_new, value_new, k_cache, v_cache):
    tok_count, seq_len, kv_heads, head_dim = k_cache.shape
    num_heads = q_heads.shape[1]
    batch, ahead = 4, 3
    buf = pltpu.VMEM((ahead + 1, batch, seq_len, kv_heads, head_dim), jnp.bfloat16)
    vmem = pl.BlockSpec(memory_space=pltpu.VMEM)
    return pl.pallas_call(
        functools.partial(attend_kernel, batch, ahead, kv_heads, num_heads // kv_heads),
        in_specs=[pl.BlockSpec(memory_space=pltpu.SMEM), vmem, vmem, vmem, pl.BlockSpec(memory_space=pltpu.HBM), pl.BlockSpec(memory_space=pltpu.HBM)],
        out_specs=vmem,
        out_shape=jax.ShapeDtypeStruct(q_heads.shape, jnp.bfloat16),
        scratch_shapes=[buf, buf, pltpu.VMEM((num_heads, seq_len * kv_heads), jnp.int32), pltpu.SemaphoreType.DMA((ahead + 1,)), pltpu.SemaphoreType.DMA((ahead + 1,))],
        compiler_params=pltpu.CompilerParams(vmem_limit_bytes=32 * MIB),
        cost_estimate=pl.CostEstimate(flops=4 * tok_count * num_heads * seq_len * kv_heads * head_dim, bytes_accessed=4 * k_cache.size, transcendentals=0),
    )(positions, q_heads, key_new, value_new, k_cache, v_cache)


def post_kernel(num_experts, steps, attn_ref, wo_ref, bo_ref, tok_ref, vec_ref, wr_ref, code_ref, x_ref, send_ref, acc_ref):
    step = pl.program_id(0)
    block = wo_ref.shape[1]
    cols = pl.ds(pl.multiple_of(step * block, block), block)
    mixed = jnp.dot(attn_ref[...], wo_ref[...], preferred_element_type=jnp.float32)
    x_mid = (tok_ref[...].astype(jnp.float32) + mixed + bo_ref[4:5, :]).astype(jnp.bfloat16)
    x_ref[...] = x_mid
    acc_ref[:, cols] = x_mid

    @pl.when(step == steps - 1)
    def _():
        h_two = layer_norm_rows(acc_ref[...].astype(jnp.float32), vec_ref[5:6, :], vec_ref[6:7, :]).astype(jnp.bfloat16)
        code = code_ref[...]
        routes = jnp.concatenate([wr_ref[...], jnp.zeros((code.shape[1] - num_experts, wr_ref.shape[1]), jnp.bfloat16)], axis=0)
        logits = lax.dot_general(h_two, routes, (((1,), (1,)), ((), ())), preferred_element_type=jnp.float32)
        hit_one = (code & 2) == 2
        hit_two = (code & 4) == 4
        keep_one = (code & 1) == 1
        keep_two = keep_one & jnp.logical_not(hit_one)

        def gate(keep, hit):
            masked = jnp.where(keep, logits, -jnp.inf)
            e_val = jnp.exp(masked - jnp.max(masked, axis=-1, keepdims=True))
            return jnp.sum(jnp.where(hit, e_val, 0.0), axis=-1, keepdims=True) / jnp.sum(e_val, axis=-1, keepdims=True)

        gates = jnp.where(hit_one, gate(keep_one, hit_one), 0.0) + jnp.where(hit_two, gate(keep_two, hit_two), 0.0)
        high = gates.astype(jnp.bfloat16).astype(jnp.float32)
        rest = gates - high
        mid = rest.astype(jnp.bfloat16).astype(jnp.float32)
        packed = high + pltpu.roll(mid, num_experts, 1) + pltpu.roll(rest - mid, 2 * num_experts, 1)
        d_model = h_two.shape[1]
        send_ref[:, :d_model] = h_two
        send_ref[:, d_model:] = packed.astype(jnp.bfloat16)


def post_attention(attn, w_out, tokens, vecs, w_router, expert_one, expert_two, eligible):
    rows, d_model = tokens.shape
    num_experts = w_router.shape[1]
    width = 128
    block = 512
    steps = d_model // block
    routes = jnp.swapaxes(w_router, 0, 1)
    ids = jnp.arange(num_experts, dtype=jnp.int32)[None, :]
    code = (eligible == 1).astype(jnp.int32) + 2 * (expert_one[:, None] == ids) + 4 * (expert_two[:, None] == ids)
    code = jnp.pad(code, ((0, 0), (0, width - num_experts)))

    def whole(arr):
        return pl.BlockSpec(arr.shape, lambda i: (0,) * arr.ndim)

    def col(i):
        return (0, i)

    return pl.pallas_call(
        functools.partial(post_kernel, num_experts, steps),
        grid=(steps,),
        in_specs=[
            whole(attn), pl.BlockSpec((attn.shape[1], block), col), pl.BlockSpec((vecs.shape[0], block), col), pl.BlockSpec((rows, block), col),
            whole(vecs), whole(routes), whole(code),
        ],
        out_specs=[pl.BlockSpec((rows, block), col), pl.BlockSpec((rows, d_model + width), lambda i: (0, 0))],
        out_shape=[jax.ShapeDtypeStruct((rows, d_model), jnp.bfloat16), jax.ShapeDtypeStruct((rows, d_model + width), jnp.bfloat16)],
        scratch_shapes=[pltpu.VMEM((rows, d_model), jnp.bfloat16)],
        compiler_params=pltpu.CompilerParams(dimension_semantics=("arbitrary",), vmem_limit_bytes=62 * MIB),
        cost_estimate=pl.CostEstimate(flops=2 * rows * d_model * d_model, bytes_accessed=2 * d_model * d_model, transcendentals=0),
    )(attn, w_out, vecs, tokens, vecs, routes, code)


STEP_ROWS = 16
DIMS = 3


def moe_kernel(num_experts, h_ref, xm_ref, wg_hbm, wu_hbm, wd_hbm, out_ref, all_ref, wg_ref, wu_ref, wd_ref, x_buf, y_buf, mate_buf, keep_refs, send_refs, recv_refs, w_sem, x_sem, own_sem, gs_sem, gr_sem, ms_sem, mr_sem, mate_s, mate_r, mate_free, red_s, red_r, red_free):
    me = lax.axis_index('ep')
    core = lax.rem(me, 2)
    chip = me // 2
    mate = chip * 2 + 1 - core
    rows, d_model = xm_ref.shape
    width = h_ref.shape[1]
    third = width // 3
    chunks = rows // STEP_ROWS
    logical = pl.DeviceIdType.MESH

    def bit(dim):
        return (chip // (1 << dim)) % 2

    def across(who, dim):
        return who + (1 - 2 * ((who // (1 << dim)) % 2)) * (1 << dim)

    def device_of(who):
        return who * 2 + core

    peers = [device_of(across(chip, dim)) for dim in range(DIMS)]

    weights = [pltpu.make_async_copy(src.at[0], dst, w_sem.at[n]) for n, (src, dst) in enumerate(((wg_hbm, wg_ref), (wu_hbm, wu_ref), (wd_hbm, wd_ref)))]
    for copy in weights:
        copy.start()
    own = pltpu.make_async_copy(h_ref, all_ref.at[me], own_sem)
    own.start()

    barrier = pltpu.get_barrier_semaphore()
    for peer in peers + [mate]:
        pl.semaphore_signal(barrier, inc=1, device_id=(peer,), device_id_type=logical)
    pl.semaphore_wait(barrier, DIMS + 1)

    def piece(owner, half, part, mine):
        cols = pl.ds(part * third, third)
        some = pl.ds(half * (rows // 2), rows // 2)
        src = h_ref.at[some, cols] if mine else all_ref.at[owner, some, cols]
        return src, all_ref.at[owner, some, cols]

    def spread(owner, half, part, slot, peer, mine):
        src, dst = piece(owner, half, part, mine)
        return pltpu.make_async_remote_copy(src, dst, gs_sem.at[half, part, slot], gr_sem.at[half, part, slot], device_id=(peer,), device_id_type=logical)

    def share(owner, half, part, slot, mine):
        src, dst = piece(owner, half, part, mine)
        return pltpu.make_async_remote_copy(src, dst, ms_sem.at[half, part, slot], mr_sem.at[half, part, slot], device_id=(mate,), device_id_type=logical)

    def held(part, step):
        whos = [chip]
        for k in range(step):
            whos = whos + [across(who, (part + k) % 3) for who in whos]
        return whos

    def wave(half, step):
        base = (1 << step) - 1
        return [spread(device_of(who), half, part, base + n, peers[(part + step) % 3], n == 0) for part in range(3) for n, who in enumerate(held(part, step))]

    def shares(half, step):
        base = 1 << step
        return [share(device_of(across(who, (part + step) % 3)), half, part, base + n, False) for part in range(3) for n, who in enumerate(held(part, step))]

    def own_shares(half):
        return [share(me, half, part, 0, True) for part in range(3)]

    def send(half, step):
        for copy in wave(half, step):
            copy.start()

    def take(half, step):
        for landed, onward in zip(wave(half, step), shares(half, step)):
            landed.wait_recv()
            onward.start()

    def shared(half):
        for copy in own_shares(half) + shares(half, 0) + shares(half, 1) + shares(half, 2):
            copy.wait_recv()

    for half in range(2):
        for copy in own_shares(half):
            copy.start()
    send(0, 0)
    send(1, 0)
    for step in range(2):
        for half in range(2):
            take(half, step)
            send(half, step + 1)
    take(0, 2)
    for copy in weights:
        copy.wait()
    own.wait()
    shared(0)

    spans = []
    at = 0
    for ref in keep_refs[:3]:
        spans.append((at, ref.shape[-1]))
        at += ref.shape[-1]

    def x_copy(c):
        return pltpu.make_async_copy(all_ref.at[:, pl.ds(pl.multiple_of(c * STEP_ROWS, STEP_ROWS), STEP_ROWS)], x_buf, x_sem)

    def mate_copy(c):
        slot = lax.rem(c, 2)
        return pltpu.make_async_remote_copy(y_buf.at[slot, :, 1 - core], mate_buf.at[slot], mate_s.at[slot], mate_r.at[slot], device_id=(mate,), device_id_type=logical)

    def red_copy(c, level, part):
        slot = lax.rem(c, 2)
        n = level * 3 + part
        return pltpu.make_async_remote_copy(send_refs[n].at[slot], recv_refs[n].at[slot], red_s.at[n, slot], red_r.at[n, slot], device_id=(peers[(part + level) % 3],), device_id_type=logical)

    def experts(c):
        slot = lax.rem(c, 2)
        x_copy(c).wait()

        @pl.when(c >= 2)
        def _():
            mate_copy(c - 2).wait_send()

        x_all = x_buf[...].reshape(num_experts * STEP_ROWS, width)
        packed = x_all[:, d_model:].astype(jnp.float32)
        lanes = lax.broadcasted_iota(jnp.int32, packed.shape, 1)
        gate = jnp.sum(jnp.where(lanes % num_experts == me, packed, 0.0), axis=-1, keepdims=True)
        x_val = x_all[:, :d_model]
        flat = (((1,), (1,)), ((), ()))
        u_val = lax.dot_general(x_val, wg_ref[...], flat, preferred_element_type=jnp.float32)
        v_val = lax.dot_general(x_val, wu_ref[...], flat, preferred_element_type=jnp.float32)
        z_val = (u_val * jax.nn.sigmoid(u_val) * v_val).astype(jnp.bfloat16)
        block = 1024
        for n in range(d_model // block):
            cols = slice(n * block, (n + 1) * block)
            y_val = jnp.dot(z_val, wd_ref[:, cols], preferred_element_type=jnp.float32).astype(jnp.bfloat16)
            y_buf[slot, :, :, :, cols] = (gate * y_val.astype(jnp.float32)).reshape(num_experts // 2, 2, STEP_ROWS, block)

        @pl.when(c >= 2)
        def _():
            pl.semaphore_wait(mate_free, 1)

        mate_copy(c).start()

        @pl.when(c + 1 < chunks)
        def _():
            x_copy(c + 1).start()

    def give(c, level):
        for part in range(3):
            @pl.when(c >= 2)
            def _():
                pl.semaphore_wait(red_free.at[level * 3 + part], 1)

            red_copy(c, level, part).start()

    def drained(c, level):
        @pl.when(c >= 2)
        def _():
            for part in range(3):
                red_copy(c - 2, level, part).wait_send()

    def first(c):
        slot = lax.rem(c, 2)
        mate_copy(c).wait_recv()
        drained(c, 0)
        for part in range(3):
            lo, size = spans[part]
            cols = slice(lo, lo + size)
            dims = [(part + k) % 3 for k in range(3)]
            for n in range(4):
                rest = (n % 2) * (1 << dims[1]) + (n // 2) * (1 << dims[2])
                for side, refs in ((bit(dims[0]), keep_refs), (1 - bit(dims[0]), send_refs)):
                    who = rest + side * (1 << dims[0])
                    refs[part][slot, n] = y_buf[slot, who, core, :, cols] + mate_buf[slot, who, :, cols]

        @pl.when(c + 2 < chunks)
        def _():
            pl.semaphore_signal(mate_free, inc=1, device_id=(mate,), device_id_type=logical)

        give(c, 0)

    def later(c, level):
        slot = lax.rem(c, 2)
        old, new = (level - 1) * 3, level * 3
        drained(c, level)
        for part in range(3):
            red_copy(c, level - 1, part).wait_recv()
            dim = (part + level) % 3
            for n in range(1 << (2 - level)):
                for side, refs in ((bit(dim), keep_refs), (1 - bit(dim), send_refs)):
                    at = n * 2 + side
                    refs[new + part][slot, n] = keep_refs[old + part][slot, at] + recv_refs[old + part][slot, at]

            @pl.when(c + 2 < chunks)
            def _():
                pl.semaphore_signal(red_free.at[old + part], inc=1, device_id=(peers[(part + level - 1) % 3],), device_id_type=logical)

        give(c, level)

    def last(c):
        slot = lax.rem(c, 2)
        here = pl.ds(pl.multiple_of(c * STEP_ROWS, STEP_ROWS), STEP_ROWS)
        for part in range(3):
            red_copy(c, 2, part).wait_recv()
            lo, size = spans[part]
            cols = slice(lo, lo + size)
            y_sum = keep_refs[6 + part][slot, 0] + recv_refs[6 + part][slot, 0]
            out_ref[here, cols] = (xm_ref[here, cols].astype(jnp.float32) + y_sum).astype(jnp.bfloat16)

            @pl.when(c + 2 < chunks)
            def _():
                pl.semaphore_signal(red_free.at[6 + part], inc=1, device_id=(peers[(part + 2) % 3],), device_id_type=logical)

    x_copy(0).start()

    def turn(i, carry):
        @pl.when(i == 2)
        def _():
            take(1, 2)

        @pl.when(i == chunks // 2 - 1)
        def _():
            shared(1)

        @pl.when(i < chunks)
        def _():
            experts(i)

        @pl.when((i >= 1) & (i - 1 < chunks))
        def _():
            first(i - 1)

        @pl.when(i >= 4)
        def _():
            last(i - 4)

        @pl.when((i >= 3) & (i - 3 < chunks))
        def _():
            later(i - 3, 2)

        @pl.when((i >= 2) & (i - 2 < chunks))
        def _():
            later(i - 2, 1)

        return carry

    lax.fori_loop(0, chunks + 4, turn, 0)
    for half in range(2):
        for copy in own_shares(half) + shares(half, 0) + shares(half, 1) + shares(half, 2) + wave(half, 0) + wave(half, 1) + wave(half, 2):
            copy.wait_send()
    for c in (chunks - 2, chunks - 1):
        mate_copy(c).wait_send()
        for level in range(3):
            for part in range(3):
                red_copy(c, level, part).wait_send()


def moe_layer(h_rows, x_mid, w_gate, w_up, w_down, num_experts):
    rows, width = h_rows.shape
    d_ff, d_model = w_down.shape[1:]
    unit = d_model // 128
    sizes = [128 * (unit // 3 + (1 if part < unit % 3 else 0)) for part in range(3)]
    chips = num_experts // 2
    f32 = jnp.float32

    def level_bufs():
        return [pltpu.VMEM((2, chips >> (level + 1), STEP_ROWS, sizes[part]), f32) for level in range(3) for part in range(3)]

    vmem = pl.BlockSpec(memory_space=pltpu.VMEM)
    hbm = pl.BlockSpec(memory_space=pltpu.HBM)
    dma = pltpu.SemaphoreType.DMA
    regular = pltpu.SemaphoreType.REGULAR
    out, _ = pl.pallas_call(
        functools.partial(moe_kernel, num_experts),
        in_specs=[vmem, vmem, hbm, hbm, hbm],
        out_specs=[vmem, hbm],
        out_shape=[jax.ShapeDtypeStruct((rows, d_model), jnp.bfloat16), jax.ShapeDtypeStruct((num_experts, rows, width), jnp.bfloat16)],
        scratch_shapes=[
            pltpu.VMEM((d_ff, d_model), jnp.bfloat16), pltpu.VMEM((d_ff, d_model), jnp.bfloat16), pltpu.VMEM((d_ff, d_model), jnp.bfloat16),
            pltpu.VMEM((num_experts, STEP_ROWS, width), jnp.bfloat16),
            pltpu.VMEM((2, chips, 2, STEP_ROWS, d_model), f32),
            pltpu.VMEM((2, chips, STEP_ROWS, d_model), f32),
            level_bufs(), level_bufs(), level_bufs(),
            dma((3,)), dma, dma, dma((2, 3, 7)), dma((2, 3, 7)), dma((2, 3, 8)), dma((2, 3, 8)),
            dma((2,)), dma((2,)), regular, dma((9, 2)), dma((9, 2)), regular((9,)),
        ],
        compiler_params=pltpu.CompilerParams(collective_id=0, has_side_effects=True, vmem_limit_bytes=67043328),
        cost_estimate=pl.CostEstimate(flops=6 * rows * num_experts * d_model * d_ff, bytes_accessed=6 * d_model * d_ff, transcendentals=0),
    )(h_rows, x_mid, jnp.swapaxes(w_gate, 1, 2), jnp.swapaxes(w_up, 1, 2), w_down)
    return out


def solution(mesh):
    def local_step(tokens, k_cache, v_cache, positions, expert_one, expert_two, eligible, ln1_gain, ln1_bias, w_query, b_query, w_key, b_key, w_value, b_value, w_out, b_out, ln2_gain, ln2_bias, w_router, w_gate, w_up, w_down):
        rows, d_model = tokens.shape
        _, seq_len, kv_heads, head_dim = k_cache.shape
        num_heads = w_query.shape[1] // head_dim
        num_experts = w_router.shape[1]
        kv_dim = b_key.shape[0]
        kv_bias = jnp.concatenate([b_key, b_value, jnp.zeros((d_model - 2 * kv_dim,), b_key.dtype)])
        vecs = jnp.stack([ln1_gain, ln1_bias, b_query, kv_bias, b_out, ln2_gain, ln2_bias, ln2_bias]).astype(jnp.float32)
        cos_tab, sin_tab = rope_tables(positions, head_dim)
        q_flat, k_flat, v_flat = qkv_project(tokens, vecs, cos_tab, sin_tab, w_query, w_key, w_value, head_dim)
        key_new = k_flat.reshape(rows, kv_heads, head_dim)
        value_new = v_flat.reshape(rows, kv_heads, head_dim)
        attn = attend(positions, q_flat.reshape(rows, num_heads, head_dim), key_new, value_new, k_cache, v_cache)
        x_mid, send = post_attention(attn.reshape(rows, num_heads * head_dim), w_out, tokens, vecs, w_router, expert_one, expert_two, eligible)
        tokens_out = moe_layer(send, x_mid, w_gate, w_up, w_down, num_experts)
        return tokens_out, key_new, value_new

    row_spec = P('ep', None)
    cache_spec = P('ep', None, None, None)
    vec_spec = P('ep')
    rep_one = P(None)
    rep_two = P(None, None)
    expert_spec = P('ep', None, None)
    in_specs = (row_spec, cache_spec, cache_spec, vec_spec, vec_spec, vec_spec, row_spec, rep_one, rep_one, rep_two, rep_one, rep_two, rep_one, rep_two, rep_one, rep_two, rep_one, rep_one, rep_one, rep_two, expert_spec, expert_spec, expert_spec)
    out_specs = (row_spec, expert_spec, expert_spec)
    return jax.shard_map(local_step, mesh=mesh, in_specs=in_specs, out_specs=out_specs, check_vma=False)
```
